32 devices in a mesh: dp: 1 (over z), tp: 32 (over x, y, core).
Axes of the slice: x: 4, y: 4, z: 1, core: 2. Of those that a mesh axis runs over, the one named last changes fastest.
The devices are a block of a 4x4x8 slice.
Arguments:
- x: bfloat16 [8192, 4096], P(('dp', 'tp'))
- w_gate: bfloat16 [4096, 16384], P(None, 'tp')
- w_up: bfloat16 [4096, 16384], P(None, 'tp')
- w_down: bfloat16 [16384, 4096], P('tp')
Outputs:
- output: bfloat16 [8192, 4096], P(('dp', 'tp'))
All inputs are finite; a program needn't handle non-finite values.
Results may differ from the reference program's by a relative error of at most 0.016.
Values are sent between devices in bfloat16 or wider.
A program may use at most 768 MiB of HBM per device.

```python
import jax
import jax.numpy as jnp

ROWS = 8192
D = 4096
FF = 16384


def setup_inputs(seed: int = 0, part: int = 0) -> dict:
    kx, kg, ku, kd = jax.random.split(jax.random.key(seed), 4)
    drawn = {
        "x": jax.random.normal(jax.random.fold_in(kx, part), (ROWS, D), jnp.float32),
        "w_gate": jax.random.normal(kg, (D, FF), jnp.float32) * D**-0.5,
        "w_up": jax.random.normal(ku, (D, FF), jnp.float32) * D**-0.5,
        "w_down": jax.random.normal(kd, (FF, D), jnp.float32) * FF**-0.5,
    }
    return {k: v.astype(jnp.bfloat16) for k, v in drawn.items()}


def reference(x, w_gate, w_up, w_down):
    gate = jnp.dot(x, w_gate, preferred_element_type=jnp.float32)
    up = jnp.dot(x, w_up, preferred_element_type=jnp.float32)
    hidden = (jax.nn.silu(gate) * up).astype(jnp.bfloat16)
    return jnp.dot(hidden, w_down, preferred_element_type=jnp.float32).astype(jnp.bfloat16)
```

```python
import functools
import math

import jax
import jax.numpy as jnp
from jax import lax
from jax.experimental import pallas as pl
from jax.experimental.pallas import tpu as pltpu
from jax.sharding import PartitionSpec as P

MESH = pl.DeviceIdType.MESH
NX, NP, NU, NB = 7, 5, 3, 2


def neighbours(side):
    me = lax.axis_index("tp")
    chip, core = me // 2, me % 2
    gx, gy = chip // side, chip % side
    diagonal = (gx + gy) % side
    ahead_x = ((diagonal + 1) // side + core) % 2
    behind_x = ((side - diagonal) // side + core) % 2
    after = ((gx + ahead_x) % side) * side + (gy + 1 - ahead_x) % side
    before = ((gx + side - behind_x) % side) * side + (gy + side - 1 + behind_x) % side
    return after * 2 + core, before * 2 + core, chip * 2 + 1 - core


def kernel(
    n, x_hbm, wg_hbm, wu_hbm, wd_hbm, y_hbm,
    tok, arr, out, sib, term, acc, hid, wg, wu, wd,
    x_sem, w_sem, y_sem, tok_send, tok_recv, swap_send, swap_recv,
    out_send, out_recv, term_send, term_recv,
):
    half = x_hbm.shape[0] // 2
    q = half // 2
    depth, width = x_hbm.shape[1], wg_hbm.shape[1]
    items = n
    after, before, sibling = neighbours(math.isqrt(n // 2))
    targets = (after, before)

    def x_load(i):
        return pltpu.make_async_copy(x_hbm.at[pl.ds(i * half, half)], tok.at[i, pl.ds(0, half)], x_sem.at[i])

    loads = [
        pltpu.make_async_copy(a, b, w_sem.at[k]) for k, (a, b) in enumerate(((wg_hbm, wg), (wu_hbm, wu), (wd_hbm, wd)))
    ]

    def y_store(i):
        return pltpu.make_async_copy(out.at[i], y_hbm.at[pl.ds(i * half, half)], y_sem.at[i])

    def tok_copy(i, r):
        here, there = i % NX, (i + 2) % NX
        return pltpu.make_async_remote_copy(
            src_ref=tok.at[here, pl.ds(r * q, q)],
            dst_ref=tok.at[there, pl.ds(r * q, q)],
            send_sem=tok_send.at[r, here],
            recv_sem=tok_recv.at[r, there],
            device_id={"tp": targets[r]},
            device_id_type=MESH,
        )

    def swap_copy(i):
        slot = i % NX
        return pltpu.make_async_remote_copy(
            src_ref=tok.at[slot, pl.ds(0, half)],
            dst_ref=tok.at[slot, pl.ds(half, half)],
            send_sem=swap_send.at[slot],
            recv_sem=swap_recv.at[slot],
            device_id={"tp": sibling},
            device_id_type=MESH,
        )

    def sib_slot(i):
        return jnp.where(i < 2, i, 2 + i % NU)

    def acc_slot(i):
        return jnp.where(i < 2, i, 2 + i % NB)

    def term_copy(i):
        here, there = i % NB, sib_slot(i)
        return pltpu.make_async_remote_copy(
            src_ref=term.at[here],
            dst_ref=sib.at[there],
            send_sem=term_send.at[here],
            recv_sem=term_recv.at[there],
            device_id={"tp": sibling},
            device_id_type=MESH,
        )

    def out_copy(i, r):
        here, there = i % NB, (i + 2) % NP
        return pltpu.make_async_remote_copy(
            src_ref=out.at[here, pl.ds(r * q, q)],
            dst_ref=arr.at[there, pl.ds(r * q, q)],
            send_sem=out_send.at[r, here],
            recv_sem=out_recv.at[r, there],
            device_id={"tp": targets[r]},
            device_id_type=MESH,
        )

    for i in range(2):
        x_load(i).start()
    for load in loads:
        load.start()
    barrier = pltpu.get_barrier_semaphore()
    for device in (after, before, sibling):
        pl.semaphore_signal(barrier, inc=1, device_id={"tp": device}, device_id_type=MESH)
    pl.semaphore_wait(barrier, 3)

    def compute(i):
        slot, here, mine = i % NX, i % NB, acc_slot(i)
        step = min(256, width)
        for c in range(0, width, step):
            rows = tok[slot]
            gate = jnp.dot(rows, wg[:, c : c + step], preferred_element_type=jnp.float32)
            up = jnp.dot(rows, wu[:, c : c + step], preferred_element_type=jnp.float32)
            hid[:, c : c + step] = (jax.nn.silu(gate) * up).astype(jnp.bfloat16)
        step = min(512, depth)
        for c in range(0, depth, step):
            t = jnp.dot(hid[...], wd[:, c : c + step], preferred_element_type=jnp.float32)
            acc[mine, :, c : c + step] = t[:half]
            term[here, :, c : c + step] = t[half:].astype(jnp.bfloat16)

    def add(i, arrived):
        here, mine, theirs, slot = i % NB, i % items, i % items, i % NP
        mine, theirs = acc_slot(mine), sib_slot(theirs)
        step = min(512, depth)

        def piece(c, _):
            cols = pl.ds(pl.multiple_of(c * step, step), step)
            total = acc[mine, :, cols] + sib[theirs, :, cols].astype(jnp.float32)
            if arrived:
                total = total + arr[slot, :, cols].astype(jnp.float32)
            out[here, :, cols] = total.astype(jnp.bfloat16)
            return 0

        lax.fori_loop(0, depth // step, piece, 0)

    def tick(i, _):
        @pl.when(i < 2)
        def _():
            x_load(i).wait()

        @pl.when((i >= 2) & (i < items))
        def _():
            for r in range(2):
                tok_copy(i - 2, r).wait_recv()

        @pl.when(i < items - 2)
        def _():
            for r in range(2):
                tok_copy(i, r).start()

        @pl.when(i < items)
        def _():
            swap_copy(i).start()

        @pl.when((i >= 2) & (i < items))
        def _():
            for r in range(2):
                tok_copy(i - 2, r).wait_send()

        @pl.when((i >= 2) & (i < items + 2))
        def _():
            swap_copy(i - 2).wait_send()

        @pl.when(i == 1)
        def _():
            for load in loads:
                load.wait()

        k = i - 1

        @pl.when((k >= 0) & (k < items))
        def _():
            swap_copy(k).wait_recv()

        @pl.when((k >= 2) & (k < items + 2))
        def _():
            term_copy(k - 2).wait_send()

        @pl.when((k >= 0) & (k < items))
        def _():
            compute(k)
            term_copy(k).start()

        j = i - 2

        @pl.when(j >= 2)
        def _():
            term_copy(j % items).wait_recv()

        @pl.when(j >= 4)
        def _():
            for r in range(2):
                out_copy(j - 2, r).wait_recv()
            for r in range(2):
                out_copy(j - 2, r).wait_send()
            add(j, True)

        @pl.when((j >= 2) & (j < 4))
        def _():
            add(j, False)

        @pl.when((j >= 2) & (j < items))
        def _():
            for r in range(2):
                out_copy(j, r).start()

        @pl.when(j >= items)
        def _():
            y_store(j - items).start()

        return 0

    lax.fori_loop(0, items + 4, tick, 0)
    for i in range(2):
        y_store(i).wait()


def solution(mesh):
    n = mesh.shape["tp"]

    def step(x, w_gate, w_up, w_down):
        rows, depth = x.shape
        width = w_gate.shape[1]
        half = rows // 2
        vmem, dma = pltpu.VMEM, pltpu.SemaphoreType.DMA
        return pl.pallas_call(
            functools.partial(kernel, n),
            out_shape=jax.ShapeDtypeStruct((rows, depth), jnp.bfloat16),
            in_specs=[pl.BlockSpec(memory_space=pl.ANY)] * 4,
            out_specs=pl.BlockSpec(memory_space=pl.ANY),
            scratch_shapes=[
                vmem((NX, 2 * half, depth), jnp.bfloat16),
                vmem((NP, half, depth), jnp.bfloat16),
                vmem((NB, half, depth), jnp.bfloat16),
                vmem((2 + NU, half, depth), jnp.bfloat16),
                vmem((NB, half, depth), jnp.bfloat16),
                vmem((2 + NB, half, depth), jnp.float32),
                vmem((2 * half, width), jnp.bfloat16),
                vmem((depth, width), jnp.bfloat16),
                vmem((depth, width), jnp.bfloat16),
                vmem((width, depth), jnp.bfloat16),
                dma((2,)),
                dma((3,)),
                dma((2,)),
                dma((2, NX)),
                dma((2, NX)),
                dma((NX,)),
                dma((NX,)),
                dma((2, NB)),
                dma((2, NP)),
                dma((NB,)),
                dma((2 + NU,)),
            ],
            compiler_params=pltpu.CompilerParams(
                collective_id=0, has_side_effects=True, vmem_limit_bytes=63 * 1024 * 1024
            ),
        )(x, w_gate, w_up, w_down)

    return jax.shard_map(
        step,
        mesh=mesh,
        in_specs=(P(("dp", "tp"), None), P(None, "tp"), P(None, "tp"), P("tp", None)),
        out_specs=P(("dp", "tp"), None),
        check_vma=False,
    )
```

```python
import functools
import math

import jax
import jax.numpy as jnp
from jax import lax
from jax.experimental import pallas as pl
from jax.experimental.pallas import tpu as pltpu
from jax.sharding import PartitionSpec as P

MESH = pl.DeviceIdType.MESH
DOWN = (
    ("a", 0, None),
    ("e", 2, None),
    ("c", 1, "a"),
    ("f", 1, "e"),
    ("h", 1, "c"),
    ("g", 3, "e"),
    ("i", 0, "h"),
    ("b", 0, "a"),
    ("j", 2, "h"),
    ("d", 3, "a"),
)
HOP = {name: hop for name, hop, _ in DOWN}
TRANSIT = ("a", "e", "h")
UP = ("i", "j", "b", "h", "d", "c", "f", "g", "a", "e")
BELOW = {name: tuple(n for n, _, parent in DOWN if parent == name) for name in UP}
LANDED = {"c": 0, "f": 1, "g": 2, "i": 3, "b": 4, "j": 5, "d": 6}
ARRIVED = {"i": 0, "j": 1, "b": 2, "h": 3, "d": 4, "c": 5, "f": 6, "g": 0, "a": 1, "e": 7}
OWN = 7
HIDDEN = {"own": 0, "c": 1, "f": 2, "g": 3, "i": 4, "b": 5, "j": 6, "d": 7}
STEPS = len(DOWN)
LAG = 3
UP0 = 2 * STEPS
ROOT0 = UP0 + 2 * STEPS + 1
NS, NO, NV = 4, 3, 2


def table(index, values):
    result = values[0]
    for k, value in enumerate(values[1:], 1):
        result = jnp.where(index == k, value, result)
    return result


def kernel(
    n, x_hbm, wg_hbm, wu_hbm, wd_hbm, y_hbm, far,
    tok, swp, out, term, sib, acc, hid, wg, wu, wd,
    x_sem, w_sem, y_sem, w_send, w_recv, tok_send, tok_recv, swap_send, swap_recv,
    out_send, out_recv, term_send, term_recv,
):
    half = x_hbm.shape[0] // 2
    q = half // 2
    depth, width = x_hbm.shape[1], wg_hbm.shape[1]
    part = width // 2
    side = math.isqrt(n // 2)
    me = lax.axis_index("tp")
    chip, core = me // 2, me % 2
    gx, gy = chip // side, chip % side
    sibling = chip * 2 + 1 - core

    def neighbour(hop):
        turn = (hop + core) % 4
        dx = (1 - turn) * ((turn + 1) % 2)
        dy = (2 - turn) * (turn % 2)
        return (((gx + dx + side) % side) * side + (gy + dy + side) % side) * 2 + core

    around = [neighbour(hop) for hop in range(4)]

    def remote(src, dst, send, recv, device):
        return pltpu.make_async_remote_copy(
            src_ref=src, dst_ref=dst, send_sem=send, recv_sem=recv, device_id={"tp": device}, device_id_type=MESH
        )

    def rows(r):
        return pl.ds(r * q, q)

    def landing(name, h, r):
        if name in TRANSIT:
            return far.at[2 * TRANSIT.index(name) + h, rows(r)]
        return tok.at[2 * LANDED[name] + h, rows(r)]

    def tok_copy(t, h, r):
        name, hop, parent = DOWN[t]
        src = x_hbm.at[pl.ds(h * half + r * q, q)] if parent is None else landing(parent, h, r)
        return remote(
            src, landing(name, h, r), tok_send.at[r, 2 * t + h], tok_recv.at[r, 2 * t + h], around[(hop + 2 * r) % 4]
        )

    def swap_copy(k, h):
        item = 2 * k + h
        src = x_hbm.at[pl.ds(h * half, half)] if k == 0 else tok.at[2 * (k - 1) + h]
        return remote(src, swp.at[item % NS], swap_send.at[item % NS], swap_recv.at[item % NS], sibling)

    def out_copy(s, h, r):
        item = 2 * s + h
        name = UP[s]
        return remote(
            out.at[item % NO, rows(r)],
            tok.at[2 * ARRIVED[name] + h, rows(r)],
            out_send.at[r, item % NO],
            out_recv.at[r, item],
            around[(HOP[name] + 2 + 2 * r) % 4],
        )

    def term_copy(item):
        return remote(term.at[item % NV], sib.at[item % NV], term_send.at[item % NV], term_recv.at[item % NV], sibling)

    def root_copy(h):
        return remote(term.at[h], swp.at[h], term_send.at[h], swap_recv.at[h], sibling)

    def x_load(h):
        return pltpu.make_async_copy(x_hbm.at[pl.ds(h * half, half)], tok.at[2 * OWN + h], x_sem.at[h])

    def y_store(h):
        slot = (ROOT0 - UP0 + h) % NO
        return pltpu.make_async_copy(out.at[slot], y_hbm.at[pl.ds(h * half, half)], y_sem.at[h])

    loads = []
    gifts = []
    for r in range(2):
        cols = pl.ds(r * part, part)
        theirs = pl.ds(width + r * part, part)
        for k, (a, b) in enumerate(((wg_hbm, wg), (wu_hbm, wu))):
            loads.append(pltpu.make_async_copy(a.at[:, cols], b.at[r], w_sem.at[2 * k + r]))
            gifts.append(remote(a.at[:, cols], b.at[2 + r], w_send.at[r, k], w_recv.at[r, k], around[2 * r]))
        gifts.append(remote(wd_hbm.at[cols], wd.at[theirs], w_send.at[r, 2], w_recv.at[r, 2], around[2 * r]))
    loads.append(pltpu.make_async_copy(wd_hbm, wd.at[pl.ds(0, width)], w_sem.at[4]))

    barrier = pltpu.get_barrier_semaphore()
    for device in (*around, sibling):
        pl.semaphore_signal(barrier, inc=1, device_id={"tp": device}, device_id_type=MESH)
    pl.semaphore_wait(barrier, 5)
    for gift in gifts:
        gift.start()
    for h in range(2):
        x_load(h).start()
    for load in loads:
        load.start()

    def compute(k, h):
        mine = 2 * ((k + OWN) % 8) + h
        item = 2 * k + h
        theirs = item % NS
        for g in range(4):
            block = jnp.concatenate([tok[mine], swp[theirs]], axis=0)
            gate = jnp.dot(block, wg[g], preferred_element_type=jnp.float32)
            up = jnp.dot(block, wu[g], preferred_element_type=jnp.float32)
            hid[item, :, g * part : (g + 1) * part] = (jax.nn.silu(gate) * up).astype(jnp.bfloat16)

    def project(item, slot):
        step = min(512, depth)
        for c in range(0, depth, step):
            t = jnp.dot(hid[item], wd[:, c : c + step], preferred_element_type=jnp.float32)
            acc[:, c : c + step] = t[:half]
            term[slot, :, c : c + step] = t[half:].astype(jnp.bfloat16)

    def add(slot, terms, theirs, arrived, h):
        step = min(512, depth)

        def piece(c, _):
            cols = pl.ds(pl.multiple_of(c * step, step), step)
            parts = [acc[:, cols], theirs(cols).astype(jnp.float32)] if terms else []
            for name in arrived:
                parts.append(tok[2 * ARRIVED[name] + h, :, cols].astype(jnp.float32))
            total = parts[0]
            for p in parts[1:]:
                total = total + p
            out[slot, :, cols] = total.astype(jnp.bfloat16)
            return 0

        lax.fori_loop(0, depth // step, piece, 0)

    def during(i, first):
        return (i >= first) & (i < first + 2), i - first

    def tick(i, _):
        for t in range(STEPS):
            now, h = during(i, 2 * t + LAG)

            @pl.when(now)
            def _(t=t, h=h):
                for r in range(2):
                    tok_copy(t, h, r).wait_recv()

        for t in range(STEPS):
            now, h = during(i, 2 * t)

            @pl.when(now)
            def _(t=t, h=h):
                for r in range(2):
                    tok_copy(t, h, r).start()

            now, h = during(i, 2 * t + LAG + 1)

            @pl.when(now)
            def _(t=t, h=h):
                for r in range(2):
                    tok_copy(t, h, r).wait_send()

        for name, k in HIDDEN.items():
            first = 0 if k == 0 else 2 * [s for s, _, _ in DOWN].index(name) + LAG
            now, h = during(i, first + 2)

            @pl.when(now)
            def _(k=k, h=h):
                swap_copy(k, h).wait_send()

        for name, k in HIDDEN.items():
            first = 0 if k == 0 else 2 * [s for s, _, _ in DOWN].index(name) + LAG
            now, h = during(i, first)

            @pl.when(now)
            def _(k=k, h=h):
                swap_copy(k, h).start()

        for s, name in enumerate(UP):
            now, h = during(i, UP0 + 2 * s + LAG)

            @pl.when(now)
            def _(s=s, h=h):
                for r in range(2):
                    out_copy(s, h, r).wait_recv()
                for r in range(2):
                    out_copy(s, h, r).wait_send()

        for s, name in enumerate(UP):
            now, h = during(i, UP0 + 2 * s)

            @pl.when(now)
            def _(s=s, name=name, h=h):
                item = 2 * s + h
                terms = name not in TRANSIT
                if terms:
                    term_copy(item).wait_recv()
                    term_copy(item).wait_send()
                add(item % NO, terms, lambda cols: sib[item % NV, :, cols], BELOW[name], h)
                for r in range(2):
                    out_copy(s, h, r).start()

        now, h = during(i, ROOT0)

        @pl.when(now)
        def _(h=h):
            root_copy(h).wait_recv()
            root_copy(h).wait_send()
            add((ROOT0 - UP0 + h) % NO, True, lambda cols: swp[h, :, cols], ("a", "e"), h)
            y_store(h).start()

        @pl.when(i == 4)
        def _():
            for h in range(2):
                x_load(h).wait()
            for load in loads:
                load.wait()
            for gift in gifts:
                gift.wait_recv()

        pair = i // 2
        firsts = [2 if k == 0 else [s for s, _, _ in DOWN].index(name) + 2 for name, k in HIDDEN.items()]
        k = table(pair, [firsts.index(p) if p in firsts else -1 for p in range(max(firsts) + 1)] + [-1])
        k = jnp.where(pair <= max(firsts), k, -1)

        @pl.when(k >= 0)
        def _():
            for c in range(8):
                now, h = during(i, 2 * firsts[c])

                @pl.when(now)
                def _(c=c, h=h):
                    swap_copy(c, h).wait_recv()

            compute(k, i % 2)

        item = i + 1 - UP0
        kinds = [-1 if name in TRANSIT else HIDDEN[name] for name in UP]
        k = jnp.where((item >= 0) & (item < 2 * STEPS), table(item // 2, kinds), -1)
        last = i + 1 - ROOT0
        root = (last >= 0) & (last < 2)

        @pl.when((k >= 0) | root)
        def _():
            slot = jnp.where(root, last, item % NV)
            project(jnp.where(root, last, 2 * k + item % 2), slot)

            @pl.when(root)
            def _():
                root_copy(last).start()

            @pl.when(k >= 0)
            def _():
                term_copy(item).start()

        return 0

    lax.fori_loop(0, ROOT0 + 2, tick, 0)
    for gift in gifts:
        gift.wait_send()
    for h in range(2):
        y_store(h).wait()


def solution(mesh):
    n = mesh.shape["tp"]

    def step(x, w_gate, w_up, w_down):
        rows, depth = x.shape
        width = w_gate.shape[1]
        half, part = rows // 2, width // 2
        vmem, dma = pltpu.VMEM, pltpu.SemaphoreType.DMA
        y, _ = pl.pallas_call(
            functools.partial(kernel, n),
            out_shape=(
                jax.ShapeDtypeStruct((rows, depth), jnp.bfloat16),
                jax.ShapeDtypeStruct((2 * len(TRANSIT), half, depth), jnp.bfloat16),
            ),
            in_specs=[pl.BlockSpec(memory_space=pl.ANY)] * 4,
            out_specs=(pl.BlockSpec(memory_space=pl.ANY),) * 2,
            scratch_shapes=[
                vmem((16, half, depth), jnp.bfloat16),
                vmem((NS, half, depth), jnp.bfloat16),
                vmem((NO, half, depth), jnp.bfloat16),
                vmem((NV, half, depth), jnp.bfloat16),
                vmem((NV, half, depth), jnp.bfloat16),
                vmem((half, depth), jnp.float32),
                vmem((16, 2 * half, 2 * width), jnp.bfloat16),
                vmem((4, depth, part), jnp.bfloat16),
                vmem((4, depth, part), jnp.bfloat16),
                vmem((2 * width, depth), jnp.bfloat16),
                dma((2,)),
                dma((5,)),
                dma((2,)),
                dma((2, 3)),
                dma((2, 3)),
                dma((2, 2 * STEPS)),
                dma((2, 2 * STEPS)),
                dma((NS,)),
                dma((NS,)),
                dma((2, NO)),
                dma((2, 2 * STEPS)),
                dma((NV,)),
                dma((NV,)),
            ],
            compiler_params=pltpu.CompilerParams(
                collective_id=0, has_side_effects=True, vmem_limit_bytes=67_043_328
            ),
        )(x, w_gate, w_up, w_down)
        return y

    return jax.shard_map(
        step,
        mesh=mesh,
        in_specs=(P(("dp", "tp"), None), P(None, "tp"), P(None, "tp"), P("tp", None)),
        out_specs=P(("dp", "tp"), None),
        check_vma=False,
    )
```

```python
import functools
import math

import jax
import jax.numpy as jnp
from jax import lax
from jax.experimental import pallas as pl
from jax.experimental.pallas import tpu as pltpu
from jax.sharding import PartitionSpec as P

MESH = pl.DeviceIdType.MESH
DOWN = (
    ("a", 0, None),
    ("e", 2, None),
    ("c", 1, "a"),
    ("f", 1, "e"),
    ("h", 1, "c"),
    ("g", 3, "e"),
    ("i", 0, "h"),
    ("b", 0, "a"),
    ("j", 2, "h"),
    ("d", 3, "a"),
)
TREE = {name: (hop, parent) for name, hop, parent in DOWN}
TRANSIT = ("a", "e", "h")
ORDER = "aecfhgiFjGbIdJBHDCEA"
AT = {name: 2 * place for place, name in enumerate(ORDER)}
BELOW = {name.upper(): tuple(n.upper() for n, _, parent in DOWN if parent == name) for name, _, _ in DOWN}
LANDED = {"c": 0, "f": 1, "g": 2, "i": 3, "j": 4, "b": 5, "d": 6}
ARRIVED = {"F": 7, "G": 0, "I": 1, "J": 2, "B": 3, "H": 4, "D": 5, "C": 6, "E": 1, "A": 2}
OWN = 7
HIDDEN = {"own": 0, "c": 1, "f": 2, "g": 3, "i": 4, "j": 5, "b": 6, "d": 7}
TICKS = 2 * len(ORDER)
LAG = 4
ROOT0 = TICKS + LAG - 2
NS, NO, NV = 4, 4, 2


def table(index, values):
    result = values[0]
    for k, value in enumerate(values[1:], 1):
        result = jnp.where(index == k, value, result)
    return result


def kernel(
    n, x_hbm, wg_hbm, wu_hbm, wd_hbm, y_hbm, far,
    tok, swp, out, term, sib, acc, hid, wg, wu, wd,
    x_sem, w_sem, y_sem, w_send, w_recv, hop_send, hop_recv, swap_send, swap_recv, term_send, term_recv, free_sem,
):
    half = x_hbm.shape[0] // 2
    q = half // 2
    depth, width = x_hbm.shape[1], wg_hbm.shape[1]
    part = width // 2
    side = math.isqrt(n // 2)
    me = lax.axis_index("tp")
    chip, core = me // 2, me % 2
    gx, gy = chip // side, chip % side
    sibling = chip * 2 + 1 - core

    def neighbour(hop):
        turn = (hop + core) % 4
        dx = (1 - turn) * ((turn + 1) % 2)
        dy = (2 - turn) * (turn % 2)
        return (((gx + dx + side) % side) * side + (gy + dy + side) % side) * 2 + core

    around = [neighbour(hop) for hop in range(4)]

    def remote(src, dst, send, recv, device):
        return pltpu.make_async_remote_copy(
            src_ref=src, dst_ref=dst, send_sem=send, recv_sem=recv, device_id={"tp": device}, device_id_type=MESH
        )

    def rows(r):
        return pl.ds(r * q, q)

    def landing(name, h, r):
        if name in TRANSIT:
            return far.at[2 * TRANSIT.index(name) + h, rows(r)]
        return tok.at[2 * LANDED[name] + h, rows(r)]

    def tok_copy(name, h, r):
        hop, parent = TREE[name]
        item = AT[name] + h
        src = x_hbm.at[pl.ds(h * half + r * q, q)] if parent is None else landing(parent, h, r)
        return remote(
            src, landing(name, h, r), hop_send.at[r, item], hop_recv.at[r, item], around[(hop + 2 * r) % 4]
        )

    def swap_copy(k, h):
        item = 2 * k + h
        src = x_hbm.at[pl.ds(h * half, half)] if k == 0 else tok.at[2 * (k - 1) + h]
        return remote(src, swp.at[item % NS], swap_send.at[item % NS], swap_recv.at[item % NS], sibling)

    def sum_copy(name, h, r):
        item = AT[name] + h
        return remote(
            out.at[item % NO, rows(r)],
            tok.at[2 * ARRIVED[name] + h, rows(r)],
            hop_send.at[r, item],
            hop_recv.at[r, item],
            around[(TREE[name.lower()][0] + 2 + 2 * r) % 4],
        )

    def hop_copy(name, h, r):
        return tok_copy(name, h, r) if name in TREE else sum_copy(name, h, r)

    def term_copy(item):
        return remote(term.at[item % NV], sib.at[item % NV], term_send.at[item % NV], term_recv.at[item % NV], sibling)

    def root_copy(h):
        return remote(term.at[h], swp.at[h], term_send.at[h], swap_recv.at[h], sibling)

    def x_load(h):
        return pltpu.make_async_copy(x_hbm.at[pl.ds(h * half, half)], tok.at[2 * OWN + h], x_sem.at[h])

    def y_store(h):
        slot = (ROOT0 + h) % NO
        return pltpu.make_async_copy(out.at[slot], y_hbm.at[pl.ds(h * half, half)], y_sem.at[h])

    loads = []
    gifts = []
    for r in range(2):
        cols = pl.ds(r * part, part)
        theirs = pl.ds(width + r * part, part)
        for k, (a, b) in enumerate(((wg_hbm, wg), (wu_hbm, wu))):
            loads.append(pltpu.make_async_copy(a.at[:, cols], b.at[r], w_sem.at[2 * k + r]))
            gifts.append(remote(a.at[:, cols], b.at[2 + r], w_send.at[r, k], w_recv.at[r, k], around[2 * r]))
        gifts.append(remote(wd_hbm.at[cols], wd.at[theirs], w_send.at[r, 2], w_recv.at[r, 2], around[2 * r]))
    loads.append(pltpu.make_async_copy(wd_hbm, wd.at[pl.ds(0, width)], w_sem.at[4]))

    barrier = pltpu.get_barrier_semaphore()
    for device in (*around, sibling):
        pl.semaphore_signal(barrier, inc=1, device_id={"tp": device}, device_id_type=MESH)
    pl.semaphore_wait(barrier, 5)
    for gift in gifts[:2] + gifts[3:5]:
        gift.start()
    for h in range(2):
        x_load(h).start()
    for load in loads:
        load.start()

    def compute(k, h):
        mine = 2 * ((k + OWN) % 8) + h
        item = 2 * k + h
        theirs = item % NS
        for g in range(4):
            block = jnp.concatenate([tok[mine], swp[theirs]], axis=0)
            gate = jnp.dot(block, wg[g], preferred_element_type=jnp.float32)
            up = jnp.dot(block, wu[g], preferred_element_type=jnp.float32)
            hid[item, :, g * part : (g + 1) * part] = (jax.nn.silu(gate) * up).astype(jnp.bfloat16)

    def project(item, slot):
        step = min(512, depth)
        for c in range(0, depth, step):
            t = jnp.dot(hid[item], wd[:, c : c + step], preferred_element_type=jnp.float32)
            acc[:, c : c + step] = t[:half]
            term[slot, :, c : c + step] = t[half:].astype(jnp.bfloat16)

    def add(slot, terms, theirs, arrived, h):
        step = min(512, depth)

        def piece(c, _):
            cols = pl.ds(pl.multiple_of(c * step, step), step)
            parts = [acc[:, cols], theirs(cols).astype(jnp.float32)] if terms else []
            for name in arrived:
                parts.append(tok[2 * ARRIVED[name] + h, :, cols].astype(jnp.float32))
            total = parts[0]
            for p in parts[1:]:
                total = total + p
            out[slot, :, cols] = total.astype(jnp.bfloat16)
            return 0

        lax.fori_loop(0, depth // step, piece, 0)

    def during(i, first):
        return (i >= first) & (i < first + 2), i - first

    swaps = [(0 if k == 0 else AT[name] + LAG, k) for name, k in HIDDEN.items()]

    def tick(i, _):
        for name in ORDER:
            now, h = during(i, AT[name] + LAG)

            @pl.when(now)
            def _(name=name, h=h):
                for r in range(2):
                    hop_copy(name, h, r).wait_recv()
                for r in range(2):
                    hop_copy(name, h, r).wait_send()

        for name in ORDER:
            now, h = during(i, AT[name])

            @pl.when(now)
            def _(name=name, h=h):
                if name not in TREE:
                    terms = name.lower() not in TRANSIT
                    if terms:
                        term_copy(i).wait_recv()
                        term_copy(i).wait_send()
                    add(i % NO, terms, lambda cols: sib[i % NV, :, cols], BELOW[name], h)
                for r in range(2):
                    hop_copy(name, h, r).start()

        for first, k in swaps:
            now, h = during(i, first + 1)

            @pl.when(now)
            def _(k=k, h=h):
                swap_copy(k, h).wait_send()

            now, h = during(i, first)

            @pl.when(now)
            def _(k=k, h=h):
                swap_copy(k, h).start()

        @pl.when(i == AT["H"] + 2)
        def _():
            for r in range(2):
                pl.semaphore_signal(free_sem.at[r], inc=1, device_id={"tp": around[2 * r]}, device_id_type=MESH)

        @pl.when(i == AT["E"] - 1)
        def _():
            for r in range(2):
                pl.semaphore_wait(free_sem.at[r], 1)

        now, h = during(i, ROOT0)

        @pl.when(now)
        def _(h=h):
            root_copy(h).wait_recv()
            root_copy(h).wait_send()
            add((ROOT0 + h) % NO, True, lambda cols: swp[h, :, cols], ("A", "E"), h)
            y_store(h).start()

        @pl.when(i == 3)
        def _():
            for gift in gifts[2::3]:
                gift.start()

        @pl.when(i == 5)
        def _():
            for h in range(2):
                x_load(h).wait()
            for load in loads:
                load.wait()
            for gift in gifts[:2] + gifts[3:5]:
                gift.wait_recv()

        @pl.when(i == AT["F"] - 1)
        def _():
            for gift in gifts[2::3]:
                gift.wait_recv()

        pair = (i - 1) // 2
        firsts = [2 if name == "own" else (AT[name] + LAG) // 2 for name in HIDDEN]
        k = table(pair, [firsts.index(p) if p in firsts else -1 for p in range(max(firsts) + 1)])
        k = jnp.where((pair >= 0) & (pair <= max(firsts)), k, -1)

        @pl.when(k >= 0)
        def _():
            for c in range(8):
                now, h = during(i, 2 * firsts[c] + 1)

                @pl.when(now)
                def _(c=c, h=h):
                    swap_copy(c, h).wait_recv()

            compute(k, (i - 1) % 2)

        item = i + 1
        kinds = [HIDDEN.get(name.lower(), -1) if name.isupper() else -1 for name in ORDER]
        k = jnp.where(item < TICKS, table(item // 2, kinds), -1)
        last = item - ROOT0
        root = (last >= 0) & (last < 2)

        @pl.when((k >= 0) | root)
        def _():
            slot = jnp.where(root, last, item % NV)
            project(jnp.where(root, last, 2 * k + item % 2), slot)

            @pl.when(root)
            def _():
                root_copy(last).start()

            @pl.when(k >= 0)
            def _():
                term_copy(item).start()

        return 0

    lax.fori_loop(0, ROOT0 + 2, tick, 0)
    for gift in gifts:
        gift.wait_send()
    for h in range(2):
        y_store(h).wait()


def solution(mesh):
    n = mesh.shape["tp"]

    def step(x, w_gate, w_up, w_down):
        rows, depth = x.shape
        width = w_gate.shape[1]
        half, part = rows // 2, width // 2
        vmem, dma = pltpu.VMEM, pltpu.SemaphoreType.DMA
        y, _ = pl.pallas_call(
            functools.partial(kernel, n),
            out_shape=(
                jax.ShapeDtypeStruct((rows, depth), jnp.bfloat16),
                jax.ShapeDtypeStruct((2 * len(TRANSIT), half, depth), jnp.bfloat16),
            ),
            in_specs=[pl.BlockSpec(memory_space=pl.ANY)] * 4,
            out_specs=(pl.BlockSpec(memory_space=pl.ANY),) * 2,
            scratch_shapes=[
                vmem((16, half, depth), jnp.bfloat16),
                vmem((NS, half, depth), jnp.bfloat16),
                vmem((NO, half, depth), jnp.bfloat16),
                vmem((NV, half, depth), jnp.bfloat16),
                vmem((NV, half, depth), jnp.bfloat16),
                vmem((half, depth), jnp.float32),
                vmem((16, 2 * half, 2 * width), jnp.bfloat16),
                vmem((4, depth, part), jnp.bfloat16),
                vmem((4, depth, part), jnp.bfloat16),
                vmem((2 * width, depth), jnp.bfloat16),
                dma((2,)),
                dma((5,)),
                dma((2,)),
                dma((2, 3)),
                dma((2, 3)),
                dma((2, TICKS)),
                dma((2, TICKS)),
                dma((NS,)),
                dma((NS,)),
                dma((NV,)),
                dma((NV,)),
                pltpu.SemaphoreType.REGULAR((2,)),
            ],
            compiler_params=pltpu.CompilerParams(
                collective_id=0, has_side_effects=True, vmem_limit_bytes=67_043_328
            ),
        )(x, w_gate, w_up, w_down)
        return y

    return jax.shard_map(
        step,
        mesh=mesh,
        in_specs=(P(("dp", "tp"), None), P(None, "tp"), P(None, "tp"), P("tp", None)),
        out_specs=P(("dp", "tp"), None),
        check_vma=False,
    )
```

```python
import functools
import math

import jax
import jax.numpy as jnp
from jax import lax
from jax.experimental import pallas as pl
from jax.experimental.pallas import tpu as pltpu
from jax.sharding import PartitionSpec as P

MESH = pl.DeviceIdType.MESH
ROLES = 7
SEQ = ((3, 1), (5, 0), (4, 0), (4, 1), (2, 1), (6, 0), (3, 0), (5, 1), (2, 0), (6, 1), (1, 1), (7, 0), (1, 0), (7, 1), (0, 0), (0, 1))
TICK = (22, 23, 24, 25, 26, 27, 28, 29, 30, 31, 32, 33, 34, 35, 37, 38)
TICK0, TICKS = TICK[0], TICK[-1] + 1
PASS = (('w', 1, 27), ('v', 0, 28), ('w', 0, 33), ('v', 1, 34))
SLOT = {name: 2 * k for k, name in enumerate((4, 2, 6, 1, 7, "w", "v"))}
BELOW = {(3, 0): (4,), (5, 1): (4,)}
BELOW |= {(role, h): below for role, below in ((1, (2, "w")), (7, (6, "v")), (0, (1, 7))) for h in range(2)}
HOP = {(4, 0): "b", (4, 1): "f"} | {
    (role, h): hop for role, hop in ((3, "kb"), (5, "kf"), (2, "b"), (6, "f"), (1, "b"), (7, "f")) for h in range(2)
}
EARLY = 8
JOBS = (0, 0, 1, 1, 1, 1, 1, 0, 1, 0, 1, 0, 1, 0, 2, 2, 2, 2, 2, 2, 2, 2, 1, 1, 1, 1, 1, 1, 1, 1)
WAIT = 14
NO, NV = 5, 2


def table(index, values):
    result = values[0]
    for k, value in enumerate(values[1:], 1):
        result = jnp.where(index == k, value, result)
    return result


def kernel(
    n, x_hbm, wg_hbm, wu_hbm, wd_hbm, y_hbm, far, swp, via,
    blk, arr, out, term, sib, acc, hid, wg, wu, wd,
    w_sem, y_sem, blk_sem, w_send, w_recv, tok_send, tok_recv, swap_send, swap_recv,
    sum_send, sum_recv, via_send, via_recv, term_send, term_recv,
):
    half = x_hbm.shape[0] // 2
    depth, width = x_hbm.shape[1], wg_hbm.shape[1]
    part = width // 2
    side = math.isqrt(n // 2)
    me = lax.axis_index("tp")
    chip, core = me // 2, me % 2
    gx, gy = chip // side, chip % side
    odd = (gx + gy) % 2
    sibling = chip * 2 + 1 - core

    def device(dx, dy):
        return (((gx + dx + side) % side) * side + (gy + dy + side) % side) * 2 + core

    ring = device(1 - odd, -odd), device(-odd, 1 - odd)
    cross = device(odd - 1, odd), device(odd, odd - 1)
    around = {
        "f": jnp.where(core == 0, ring[0], ring[1]),
        "b": jnp.where(core == 0, ring[1], ring[0]),
        "kb": jnp.where(core == 0, cross[0], cross[1]),
        "kf": jnp.where(core == 0, cross[1], cross[0]),
    }

    def remote(src, dst, send, recv, target):
        return pltpu.make_async_remote_copy(
            src_ref=src, dst_ref=dst, send_sem=send, recv_sem=recv, device_id={"tp": target}, device_id_type=MESH
        )

    def own(h):
        return x_hbm.at[pl.ds(h * half, half)]

    def tok_copy(j, own_half=None):
        src = own(own_half) if own_half is not None else far.at[j - 2]
        return remote(src, far.at[j], tok_send.at[j], tok_recv.at[j], around["f"])

    def swap_copy(c, own_half=None):
        src = own(own_half) if own_half is not None else far.at[c - 2]
        return remote(src, swp.at[c], swap_send.at[c], swap_recv.at[c], sibling)

    def sum_copy(k):
        role, h = SEQ[k]
        if role in (3, 5):
            return remote(
                out.at[k % NO], via.at[role - 3 + h], sum_send.at[k], via_recv.at[role - 3 + h], around[HOP[role, h]]
            )
        return remote(
            out.at[k % NO], arr.at[SLOT[role] + h], sum_send.at[k], sum_recv.at[SLOT[role] + h], around[HOP[role, h]]
        )

    def via_in(kind, h):
        return sum_copy(SEQ.index((3 if kind == "w" else 5, h)))

    def via_copy(kind, h):
        here = (0 if kind == "w" else 2) + h
        return remote(
            via.at[here], arr.at[SLOT[kind] + h], via_send.at[here], sum_recv.at[SLOT[kind] + h],
            around["kb" if kind == "w" else "kf"],
        )

    def arrival(name, h):
        if name in ("w", "v"):
            return via_copy(name, h)
        return sum_copy(SEQ.index((name, h)))

    def term_copy(k):
        return remote(term.at[k % NV], sib.at[k % NV], term_send.at[k % NV], term_recv.at[k % NV], sibling)

    def job_block(z):
        return jnp.where(z < EARLY, z, jnp.where(z < 2 * EARLY, z - EARLY, z // 2))

    def blk_copies(z, src):
        slot = z % 2
        return (
            pltpu.make_async_copy(src, blk.at[slot, pl.ds(0, half)], blk_sem.at[slot, 0]),
            pltpu.make_async_copy(swp.at[job_block(z)], blk.at[slot, pl.ds(half, half)], blk_sem.at[slot, 1]),
        )

    def blk_load(z):
        c = job_block(z)

        @pl.when(c < 2)
        def _():
            for load in blk_copies(z, own(c)):
                load.start()

        @pl.when(c >= 2)
        def _():
            for load in blk_copies(z, far.at[c - 2]):
                load.start()

    def y_store(h):
        k = SEQ.index((0, h))
        return pltpu.make_async_copy(out.at[k % NO], y_hbm.at[pl.ds(h * half, half)], y_sem.at[h])

    loads, gifts = [], []
    for g in range(2):
        cols = pl.ds(g * part, part)
        for k, (a, b) in enumerate(((wg_hbm, wg), (wu_hbm, wu))):
            loads.append(pltpu.make_async_copy(a.at[:, cols], b.at[g], w_sem.at[2 * k + g]))
            gifts.append(
                remote(a.at[:, cols], b.at[2 + g], w_send.at[2 * k + g], w_recv.at[2 * k + g], around["kb"])
            )
    loads.append(pltpu.make_async_copy(wd_hbm, wd.at[pl.ds(0, width)], w_sem.at[4]))
    gifts.append(remote(wd_hbm, wd.at[pl.ds(width, width)], w_send.at[4], w_recv.at[4], around["kb"]))

    barrier = pltpu.get_barrier_semaphore()
    for target in (*around.values(), sibling):
        pl.semaphore_signal(barrier, inc=1, device_id={"tp": target}, device_id_type=MESH)
    pl.semaphore_wait(barrier, 5)
    for h in range(2):
        tok_copy(h, h).start()
    for gift in gifts:
        gift.start()
    for h in range(2):
        swap_copy(h, h).start()
    for load in loads:
        load.start()

    def compute(z):
        c, late = job_block(z), jnp.where(z < EARLY, 0, jnp.where(z < 2 * EARLY, 1, z % 2))
        for g in range(2):
            block = blk[z % 2]
            group = 2 * late + g
            gate = jnp.dot(block, wg[group], preferred_element_type=jnp.float32)
            up = jnp.dot(block, wu[group], preferred_element_type=jnp.float32)
            cols = pl.ds(pl.multiple_of(group * part, part), part)
            hid[c, :, cols] = (jax.nn.silu(gate) * up).astype(jnp.bfloat16)

    def project(item, slot):
        step = min(512, depth)
        for c in range(0, depth, step):
            t = jnp.dot(hid[item], wd[:, c : c + step], preferred_element_type=jnp.float32)
            acc[:, c : c + step] = t[:half]
            term[slot, :, c : c + step] = t[half:].astype(jnp.bfloat16)

    def add(k):
        role, h = SEQ[k]
        step = min(512, depth)

        def piece(c, _):
            cols = pl.ds(pl.multiple_of(c * step, step), step)
            total = acc[:, cols] + sib[k % NV, :, cols].astype(jnp.float32)
            for name in BELOW.get((role, h), ()):
                total = total + arr[SLOT[name] + h, :, cols].astype(jnp.float32)
            out[k % NO, :, cols] = total.astype(jnp.bfloat16)
            return 0

        lax.fori_loop(0, depth // step, piece, 0)

    blocks = 2 * ROLES

    def tick(i, _):
        j = i // 2
        due = i % 2 == 0

        @pl.when(due & (j < blocks))
        def _():
            tok_copy(j, 0).wait_recv()

        @pl.when(due & (j < blocks - 2))
        def _():
            tok_copy(j + 2).start()

        @pl.when(due & (j < blocks))
        def _():
            swap_copy(j + 2).start()

        for kind, h, when in PASS:

            @pl.when(i == when)
            def _(kind=kind, h=h):
                via_in(kind, h).wait_recv()
                via_copy(kind, h).start()

        for k, (role, h) in enumerate(SEQ):

            @pl.when(i == TICK[k])
            def _(k=k, role=role, h=h):
                for name in BELOW.get((role, h), ()):
                    arrival(name, h).wait_recv()
                if k >= NO:
                    sum_copy(k - NO).wait_send()
                term_copy(k).wait_recv()
                term_copy(k).wait_send()
                add(k)
                if role:
                    sum_copy(k).start()
                else:
                    y_store(h).start()

        @pl.when(i == [k for k, count in enumerate(JOBS) if count][0])
        def _():
            for load in loads:
                load.wait()

        @pl.when(i == WAIT)
        def _():
            for gift in gifts[:-1]:
                gift.wait_recv()

        first = table(i, [sum(JOBS[:k]) for k in range(len(JOBS))])
        count = jnp.where(i < len(JOBS), table(i, JOBS), 0)

        def job(z, _):
            @pl.when(z < EARLY)
            def _():
                swap_copy(z, 0).wait_recv()
                blk_load(z)

            for load in blk_copies(z, own(0)):
                load.wait()

            @pl.when((z + 1 >= 2 * EARLY) & (z + 1 < 2 * (blocks + 2)) & (z % 2 == 1))
            def _():
                swap_copy(job_block(z + 1), 0).wait_recv()

            @pl.when((z + 1 >= EARLY) & (z + 1 < 2 * (blocks + 2)))
            def _():
                blk_load(z + 1)

            compute(z)
            return 0

        lax.fori_loop(first, first + count, job, 0)

        @pl.when(i == TICK0 - 1)
        def _():
            gifts[-1].wait_recv()

        places = {t - 1: k for k, t in enumerate(TICK)}
        k = jnp.where(i >= TICK0 - 1, table(i - TICK0 + 1, [places.get(t, -1) for t in range(TICK0 - 1, TICKS)]), -1)

        @pl.when(k >= 0)
        def _():
            project(table(k, [2 * role + h for role, h in SEQ]), k % NV)
            term_copy(k).start()

        return 0

    lax.fori_loop(0, TICKS, tick, 0)
    for gift in gifts:
        gift.wait_send()
    for j in range(2):
        tok_copy(j, j).wait_send()
        swap_copy(j, j).wait_send()
    for j in range(2, blocks):
        tok_copy(j).wait_send()
    for c in range(2, blocks + 2):
        swap_copy(c).wait_send()
    for k, (role, _) in enumerate(SEQ):
        if role and k >= len(SEQ) - NO:
            sum_copy(k).wait_send()
    for kind, h, _ in PASS:
        via_copy(kind, h).wait_send()
    for h in range(2):
        y_store(h).wait()


def solution(mesh):
    n = mesh.shape["tp"]

    def step(x, w_gate, w_up, w_down):
        rows, depth = x.shape
        width = w_gate.shape[1]
        half, part = rows // 2, width // 2
        vmem, dma = pltpu.VMEM, pltpu.SemaphoreType.DMA
        blocks = 2 * ROLES
        out = pl.pallas_call(
            functools.partial(kernel, n),
            out_shape=(
                jax.ShapeDtypeStruct((rows, depth), jnp.bfloat16),
                jax.ShapeDtypeStruct((blocks, half, depth), jnp.bfloat16),
                jax.ShapeDtypeStruct((blocks + 2, half, depth), jnp.bfloat16),
                jax.ShapeDtypeStruct((4, half, depth), jnp.bfloat16),
            ),
            in_specs=[pl.BlockSpec(memory_space=pl.ANY)] * 4,
            out_specs=(pl.BlockSpec(memory_space=pl.ANY),) * 4,
            scratch_shapes=[
                vmem((2, 2 * half, depth), jnp.bfloat16),
                vmem((2 * len(SLOT), half, depth), jnp.bfloat16),
                vmem((NO, half, depth), jnp.bfloat16),
                vmem((NV, half, depth), jnp.bfloat16),
                vmem((NV, half, depth), jnp.bfloat16),
                vmem((half, depth), jnp.float32),
                vmem((blocks + 2, 2 * half, 2 * width), jnp.bfloat16),
                vmem((4, depth, part), jnp.bfloat16),
                vmem((4, depth, part), jnp.bfloat16),
                vmem((2 * width, depth), jnp.bfloat16),
                dma((5,)),
                dma((2,)),
                dma((2, 2)),
                dma((5,)),
                dma((5,)),
                dma((blocks,)),
                dma((blocks,)),
                dma((blocks + 2,)),
                dma((blocks + 2,)),
                dma((len(SEQ),)),
                dma((2 * len(SLOT),)),
                dma((4,)),
                dma((4,)),
                dma((NV,)),
                dma((NV,)),
            ],
            compiler_params=pltpu.CompilerParams(
                collective_id=0, has_side_effects=True, vmem_limit_bytes=67_043_328
            ),
        )(x, w_gate, w_up, w_down)
        return out[0]

    return jax.shard_map(
        step,
        mesh=mesh,
        in_specs=(P(("dp", "tp"), None), P(None, "tp"), P(None, "tp"), P("tp", None)),
        out_specs=P(("dp", "tp"), None),
        check_vma=False,
    )
```

```python
import functools
import math

import jax
import jax.numpy as jnp
from jax import lax
from jax.experimental import pallas as pl
from jax.experimental.pallas import tpu as pltpu
from jax.sharding import PartitionSpec as P

MESH = pl.DeviceIdType.MESH
ROLES = 7
SEQ = ((3, 1), (5, 0), (4, 0), (4, 1), (2, 1), (6, 0), (3, 0), (5, 1), (2, 0), (6, 1), (1, 1), (7, 0), (1, 0), (7, 1), (0, 0), (0, 1))
TICK = (22, 23, 24, 25, 26, 27, 28, 29, 30, 31, 32, 33, 34, 35, 37, 38)
TICK0, TICKS = TICK[0], TICK[-1] + 1
PASS = (('w', 1, 27), ('v', 0, 28), ('w', 0, 33), ('v', 1, 34))
SLOT = {name: 2 * k for k, name in enumerate((4, 2, 6, 1, 7, "w", "v"))}
BELOW = {(3, 0): (4,), (5, 1): (4,)}
BELOW |= {(role, h): below for role, below in ((1, (2, "w")), (7, (6, "v")), (0, (1, 7))) for h in range(2)}
HOP = {(4, 0): "b", (4, 1): "f"} | {
    (role, h): hop for role, hop in ((3, "kb"), (5, "kf"), (2, "b"), (6, "f"), (1, "b"), (7, "f")) for h in range(2)
}
EARLY = 8
JOBS = (0, 0, 1, 1, 1, 1, 1, 0, 1, 0, 1, 0, 1, 0, 2, 2, 2, 2, 2, 2, 2, 2, 1, 1, 1, 1, 1, 1, 1, 1)
WAIT = 14
NO, NV = 5, 2


def table(index, values):
    result = values[0]
    for k, value in enumerate(values[1:], 1):
        result = jnp.where(index == k, value, result)
    return result


def kernel(
    n, x_hbm, wg_hbm, wu_hbm, wd_hbm, y_hbm, far, swp, via,
    blk, arr, out, term, sib, acc, hid, wg, wu, wd,
    w_sem, y_sem, blk_sem, w_send, w_recv, tok_send, tok_recv, swap_send, swap_recv,
    sum_send, sum_recv, via_send, via_recv, term_send, term_recv,
):
    half = x_hbm.shape[0] // 2
    depth, width = x_hbm.shape[1], wg_hbm.shape[1]
    part = width // 2
    side = math.isqrt(n // 2)
    me = lax.axis_index("tp")
    chip, core = me // 2, me % 2
    gx, gy = chip // side, chip % side
    odd = (gx + gy) % 2
    sibling = chip * 2 + 1 - core

    def device(dx, dy):
        return (((gx + dx + side) % side) * side + (gy + dy + side) % side) * 2 + core

    ring = device(1 - odd, -odd), device(-odd, 1 - odd)
    cross = device(odd - 1, odd), device(odd, odd - 1)
    around = {
        "f": jnp.where(core == 0, ring[0], ring[1]),
        "b": jnp.where(core == 0, ring[1], ring[0]),
        "kb": jnp.where(core == 0, cross[0], cross[1]),
        "kf": jnp.where(core == 0, cross[1], cross[0]),
    }

    def remote(src, dst, send, recv, target):
        return pltpu.make_async_remote_copy(
            src_ref=src, dst_ref=dst, send_sem=send, recv_sem=recv, device_id={"tp": target}, device_id_type=MESH
        )

    def own(h):
        return x_hbm.at[pl.ds(h * half, half)]

    def tok_copy(j, own_half=None):
        src = own(own_half) if own_half is not None else far.at[j - 2]
        return remote(src, far.at[j], tok_send.at[j], tok_recv.at[j], around["f"])

    def swap_copy(c, own_half=None):
        src = own(own_half) if own_half is not None else far.at[c - 2]
        return remote(src, swp.at[c], swap_send.at[c], swap_recv.at[c], sibling)

    def sum_copy(k):
        role, h = SEQ[k]
        if role in (3, 5):
            return remote(
                out.at[k % NO], via.at[role - 3 + h], sum_send.at[k], via_recv.at[role - 3 + h], around[HOP[role, h]]
            )
        return remote(
            out.at[k % NO], arr.at[SLOT[role] + h], sum_send.at[k], sum_recv.at[SLOT[role] + h], around[HOP[role, h]]
        )

    def via_in(kind, h):
        return sum_copy(SEQ.index((3 if kind == "w" else 5, h)))

    def via_copy(kind, h):
        here = (0 if kind == "w" else 2) + h
        return remote(
            via.at[here], arr.at[SLOT[kind] + h], via_send.at[here], sum_recv.at[SLOT[kind] + h],
            around["kb" if kind == "w" else "kf"],
        )

    def arrival(name, h):
        if name in ("w", "v"):
            return via_copy(name, h)
        return sum_copy(SEQ.index((name, h)))

    def term_copy(k):
        return remote(term.at[k % NV], sib.at[k % NV], term_send.at[k % NV], term_recv.at[k % NV], sibling)

    def job_block(z):
        return jnp.where(z < EARLY, z, jnp.where(z < 2 * EARLY, z - EARLY, z // 2))

    def blk_copies(z, src):
        slot = z % 2
        return (
            pltpu.make_async_copy(src, blk.at[slot, pl.ds(0, half)], blk_sem.at[slot, 0]),
            pltpu.make_async_copy(swp.at[job_block(z)], blk.at[slot, pl.ds(half, half)], blk_sem.at[slot, 1]),
        )

    def blk_load(z):
        c = job_block(z)

        @pl.when(c < 2)
        def _():
            for load in blk_copies(z, own(c)):
                load.start()

        @pl.when(c >= 2)
        def _():
            for load in blk_copies(z, far.at[c - 2]):
                load.start()

    def y_store(h):
        k = SEQ.index((0, h))
        return pltpu.make_async_copy(out.at[k % NO], y_hbm.at[pl.ds(h * half, half)], y_sem.at[h])

    loads, gifts = [], []
    for g in range(2):
        cols = pl.ds(g * part, part)
        for k, (a, b) in enumerate(((wg_hbm, wg), (wu_hbm, wu))):
            loads.append(pltpu.make_async_copy(a.at[:, cols], b.at[g], w_sem.at[2 * k + g]))
            gifts.append(
                remote(a.at[:, cols], b.at[2 + g], w_send.at[2 * k + g], w_recv.at[2 * k + g], around["kb"])
            )
    loads.append(pltpu.make_async_copy(wd_hbm, wd.at[pl.ds(0, width)], w_sem.at[4]))
    gifts.append(remote(wd_hbm, wd.at[pl.ds(width, width)], w_send.at[4], w_recv.at[4], around["kb"]))

    for load in loads:
        load.start()
    barrier = pltpu.get_barrier_semaphore()
    for target in (*around.values(), sibling):
        pl.semaphore_signal(barrier, inc=1, device_id={"tp": target}, device_id_type=MESH)
    pl.semaphore_wait(barrier, 5)
    for h in range(2):
        tok_copy(h, h).start()
    for gift in gifts:
        gift.start()
    for h in range(2):
        swap_copy(h, h).start()

    def compute(z):
        c, late = job_block(z), jnp.where(z < EARLY, 0, jnp.where(z < 2 * EARLY, 1, z % 2))
        for g in range(2):
            block = blk[z % 2]
            group = 2 * late + g
            gate = jnp.dot(block, wg[group], preferred_element_type=jnp.float32)
            up = jnp.dot(block, wu[group], preferred_element_type=jnp.float32)
            cols = pl.ds(pl.multiple_of(group * part, part), part)
            hid[c, :, cols] = (jax.nn.silu(gate) * up).astype(jnp.bfloat16)

    def project(item, slot):
        step = min(512, depth)
        for c in range(0, depth, step):
            t = jnp.dot(hid[item], wd[:, c : c + step], preferred_element_type=jnp.float32)
            acc[:, c : c + step] = t[:half]
            term[slot, :, c : c + step] = t[half:].astype(jnp.bfloat16)

    def add(k):
        role, h = SEQ[k]
        step = min(512, depth)

        def piece(c, _):
            cols = pl.ds(pl.multiple_of(c * step, step), step)
            total = acc[:, cols] + sib[k % NV, :, cols].astype(jnp.float32)
            for name in BELOW.get((role, h), ()):
                total = total + arr[SLOT[name] + h, :, cols].astype(jnp.float32)
            out[k % NO, :, cols] = total.astype(jnp.bfloat16)
            return 0

        lax.fori_loop(0, depth // step, piece, 0)

    blocks = 2 * ROLES

    def tick(i, _):
        j = i // 2
        due = i % 2 == 0

        @pl.when(due & (j < blocks))
        def _():
            tok_copy(j, 0).wait_recv()

        @pl.when(due & (j < blocks - 2))
        def _():
            tok_copy(j + 2).start()

        @pl.when(due & (j < blocks))
        def _():
            swap_copy(j + 2).start()

        for kind, h, when in PASS:

            @pl.when(i == when)
            def _(kind=kind, h=h):
                via_in(kind, h).wait_recv()
                via_copy(kind, h).start()

        for k, (role, h) in enumerate(SEQ):

            @pl.when(i == TICK[k])
            def _(k=k, role=role, h=h):
                for name in BELOW.get((role, h), ()):
                    arrival(name, h).wait_recv()
                if k >= NO:
                    sum_copy(k - NO).wait_send()
                term_copy(k).wait_recv()
                term_copy(k).wait_send()
                add(k)
                if role:
                    sum_copy(k).start()
                else:
                    y_store(h).start()

        @pl.when(i == [k for k, count in enumerate(JOBS) if count][0])
        def _():
            for load in loads:
                load.wait()

        @pl.when(i == WAIT)
        def _():
            for gift in gifts[:-1]:
                gift.wait_recv()

        first = table(i, [sum(JOBS[:k]) for k in range(len(JOBS))])
        count = jnp.where(i < len(JOBS), table(i, JOBS), 0)

        def job(z, _):
            @pl.when(z < EARLY)
            def _():
                swap_copy(z, 0).wait_recv()
                blk_load(z)

            for load in blk_copies(z, own(0)):
                load.wait()

            @pl.when((z + 1 >= 2 * EARLY) & (z + 1 < 2 * (blocks + 2)) & (z % 2 == 1))
            def _():
                swap_copy(job_block(z + 1), 0).wait_recv()

            @pl.when((z + 1 >= EARLY) & (z + 1 < 2 * (blocks + 2)))
            def _():
                blk_load(z + 1)

            compute(z)
            return 0

        lax.fori_loop(first, first + count, job, 0)

        @pl.when(i == TICK0 - 1)
        def _():
            gifts[-1].wait_recv()

        places = {t - 1: k for k, t in enumerate(TICK)}
        k = jnp.where(i >= TICK0 - 1, table(i - TICK0 + 1, [places.get(t, -1) for t in range(TICK0 - 1, TICKS)]), -1)

        @pl.when(k >= 0)
        def _():
            project(table(k, [2 * role + h for role, h in SEQ]), k % NV)
            term_copy(k).start()

        return 0

    lax.fori_loop(0, TICKS, tick, 0)
    for gift in gifts:
        gift.wait_send()
    for j in range(2):
        tok_copy(j, j).wait_send()
        swap_copy(j, j).wait_send()
    for j in range(2, blocks):
        tok_copy(j).wait_send()
    for c in range(2, blocks + 2):
        swap_copy(c).wait_send()
    for k, (role, _) in enumerate(SEQ):
        if role and k >= len(SEQ) - NO:
            sum_copy(k).wait_send()
    for kind, h, _ in PASS:
        via_copy(kind, h).wait_send()
    for h in range(2):
        y_store(h).wait()


def solution(mesh):
    n = mesh.shape["tp"]

    def step(x, w_gate, w_up, w_down):
        rows, depth = x.shape
        width = w_gate.shape[1]
        half, part = rows // 2, width // 2
        vmem, dma = pltpu.VMEM, pltpu.SemaphoreType.DMA
        blocks = 2 * ROLES
        out = pl.pallas_call(
            functools.partial(kernel, n),
            out_shape=(
                jax.ShapeDtypeStruct((rows, depth), jnp.bfloat16),
                jax.ShapeDtypeStruct((blocks, half, depth), jnp.bfloat16),
                jax.ShapeDtypeStruct((blocks + 2, half, depth), jnp.bfloat16),
                jax.ShapeDtypeStruct((4, half, depth), jnp.bfloat16),
            ),
            in_specs=[pl.BlockSpec(memory_space=pl.ANY)] * 4,
            out_specs=(pl.BlockSpec(memory_space=pl.ANY),) * 4,
            scratch_shapes=[
                vmem((2, 2 * half, depth), jnp.bfloat16),
                vmem((2 * len(SLOT), half, depth), jnp.bfloat16),
                vmem((NO, half, depth), jnp.bfloat16),
                vmem((NV, half, depth), jnp.bfloat16),
                vmem((NV, half, depth), jnp.bfloat16),
                vmem((half, depth), jnp.float32),
                vmem((blocks + 2, 2 * half, 2 * width), jnp.bfloat16),
                vmem((4, depth, part), jnp.bfloat16),
                vmem((4, depth, part), jnp.bfloat16),
                vmem((2 * width, depth), jnp.bfloat16),
                dma((5,)),
                dma((2,)),
                dma((2, 2)),
                dma((5,)),
                dma((5,)),
                dma((blocks,)),
                dma((blocks,)),
                dma((blocks + 2,)),
                dma((blocks + 2,)),
                dma((len(SEQ),)),
                dma((2 * len(SLOT),)),
                dma((4,)),
                dma((4,)),
                dma((NV,)),
                dma((NV,)),
            ],
            compiler_params=pltpu.CompilerParams(
                collective_id=0, has_side_effects=True, vmem_limit_bytes=67_043_328
            ),
        )(x, w_gate, w_up, w_down)
        return out[0]

    return jax.shard_map(
        step,
        mesh=mesh,
        in_specs=(P(("dp", "tp"), None), P(None, "tp"), P(None, "tp"), P("tp", None)),
        out_specs=P(("dp", "tp"), None),
        check_vma=False,
    )
```
